32 devices in a mesh: part: 1 (over z), ray: 4 (over y), pix: 8 (over x, core).
Axes of the slice: x: 4, y: 4, z: 1, core: 2. Of those that a mesh axis runs over, the one named last changes fastest.
The devices are a block of a 4x4x8 slice.
Arguments:
- sys_mat: bfloat16 [23040, 9216], P('ray', 'pix')
- x_init: float32 [9216, 128], P('pix', 'part')
- sinogram: float32 [23040, 128], P('ray', 'part')
- row_inv: float32 [23040], P('ray')
- col_inv: float32 [9216], P('pix')
- relaxation: float32 [], replicated
Outputs:
- output 1: float32 [9216, 128], P('pix', 'part')
- output 2: float32 [23040, 128], P('ray', 'part')
- output 3: float32 [6, 128], P(None, 'part')
All inputs are finite; a program needn't handle non-finite values.
Results may differ from the reference program's by a relative error of at most 0.001.
Values are sent between devices in bfloat16 or wider.
A program may use at most 768 MiB of HBM per device.

```python
import jax
import jax.numpy as jnp
from jax import lax

RAYS = 23040
PIXELS = 9216
SLICES = 128
SWEEPS = 6
ROW_BLOCK = 128
FIELD_MODES = 8


def smooth_modes():
    grid_pos = (jnp.arange(PIXELS, dtype=jnp.float32) + 0.5) / PIXELS
    mode_ids = jnp.arange(1, FIELD_MODES + 1, dtype=jnp.float32)
    phase_arg = 2.0 * jnp.pi * grid_pos[:, None] * mode_ids[None, :]
    mode_basis = jnp.concatenate([jnp.cos(phase_arg), jnp.sin(phase_arg)], axis=1)
    return grid_pos, mode_basis, jnp.concatenate([mode_ids, mode_ids])


def draw_image(key_img, mode_basis, mode_ids):
    key_off, key_coef, key_white = jax.random.split(key_img, 3)
    offsets = 0.3 * jax.random.normal(key_off, (SLICES,), jnp.float32)
    mode_coef = jax.random.normal(key_coef, (2 * FIELD_MODES, SLICES), jnp.float32) * (0.5 / jnp.sqrt(mode_ids))[:, None]
    white_noise = 0.1 * jax.random.normal(key_white, (PIXELS, SLICES), jnp.float32)
    smooth_part = jnp.dot(mode_basis, mode_coef, preferred_element_type=jnp.float32)
    return 1.0 + offsets[None, :] + smooth_part + white_noise


def setup_inputs(seed: int = 0, part: int = 0) -> dict:
    base_key = jax.random.key(seed)
    key_mat, key_row, key_col, key_relax = jax.random.split(base_key, 4)
    part_key = jax.random.fold_in(jax.random.key(seed + 1), part)
    key_start, key_truth, key_noise = jax.random.split(part_key, 3)
    grid_pos, mode_basis, mode_ids = smooth_modes()
    x_init = draw_image(key_start, mode_basis, mode_ids)
    x_true = draw_image(key_truth, mode_basis, mode_ids)

    def row_block(col_sum, block_id):
        ray_pos = (block_id.astype(jnp.float32) * ROW_BLOCK + jnp.arange(ROW_BLOCK, dtype=jnp.float32) + 0.5) / RAYS
        scaled_dist = (ray_pos[:, None] - grid_pos[None, :]) / 0.03
        jitter = jax.random.uniform(jax.random.fold_in(key_mat, block_id), (ROW_BLOCK, PIXELS), jnp.float32)
        block_val = ((0.02 + jnp.exp(-scaled_dist * scaled_dist)) * (0.5 + jitter)).astype(jnp.bfloat16)
        block_f32 = block_val.astype(jnp.float32)
        clean_rows = jnp.dot(block_f32, x_true, preferred_element_type=jnp.float32)
        new_sum = col_sum + jnp.sum(block_f32, axis=0)
        return new_sum, (block_val, clean_rows, jnp.sum(block_f32, axis=1))

    col_sum, (blocks, clean_sino, row_sum) = lax.scan(row_block, jnp.zeros((PIXELS,), jnp.float32), jnp.arange(RAYS // ROW_BLOCK))
    sys_mat = blocks.reshape(RAYS, PIXELS)
    row_sum = row_sum.reshape(RAYS)
    sino_noise = jax.random.normal(key_noise, (RAYS, SLICES), jnp.float32)
    sinogram = clean_sino.reshape(RAYS, SLICES) + 0.02 * row_sum[:, None] * sino_noise
    row_inv = jax.random.uniform(key_row, (RAYS,), jnp.float32, minval=0.5, maxval=1.0) / row_sum
    col_inv = jax.random.uniform(key_col, (PIXELS,), jnp.float32, minval=0.5, maxval=1.0) / col_sum
    relaxation = jax.random.uniform(key_relax, (), jnp.float32, minval=0.8, maxval=1.6)
    return {"sys_mat": sys_mat, "x_init": x_init, "sinogram": sinogram, "row_inv": row_inv, "col_inv": col_inv, "relaxation": relaxation}


def reference(sys_mat, x_init, sinogram, row_inv, col_inv, relaxation):
    def one_sweep(state_pair, unused):
        image_cur, prev_resid = state_pair
        projected = jnp.dot(sys_mat, image_cur.astype(jnp.bfloat16), preferred_element_type=jnp.float32)
        residual = row_inv[:, None] * (sinogram - projected)
        sq_norm = jnp.sum(residual * residual, axis=0) / RAYS
        back_proj = jnp.dot(residual.astype(jnp.bfloat16).T, sys_mat, preferred_element_type=jnp.float32).T
        image_cur = image_cur + relaxation * col_inv[:, None] * back_proj
        return (image_cur, residual), sq_norm

    init_state = (x_init, jnp.zeros_like(sinogram))
    (x_final, resid_last), sq_norms = lax.scan(one_sweep, init_state, None, length=SWEEPS)
    return x_final, resid_last, sq_norms
```

```python
import functools

import jax
import jax.numpy as jnp
from jax import lax
from jax.experimental import pallas as pl
from jax.experimental.pallas import tpu as pltpu
from jax.sharding import PartitionSpec as P

SWEEPS = 6
MESH = pl.DeviceIdType.MESH
F32 = jnp.float32
BF16 = jnp.bfloat16

CHUNKS = ((0, 240, 128), (240, 240, 112), (480, 240, 128))


class Lazy:
    def __init__(self, makers):
        self.makers = makers

    def __getitem__(self, key):
        return self.makers[key]()

    def values(self):
        return [make() for make in self.makers.values()]


def _kernel(ring_x, ring_y, ray_total, a_hbm, x_in, b_hbm, rinv, cinv, lam, x_out, r_out, s_out,
            a_v, b_v, ps, pd, ss, q, fl, fr, rall, rf, gt, qy, fyl, fyr, xs, xb, xf, xn, sqv, sqr, sqc,
            a_sem, b_sem, o_sem, send, recv):
    rp = ss.shape[1]
    cy = gt.shape[1]
    width = gt.shape[2]
    n_x, n_y = ring_x // 2, ring_y
    pix = lax.axis_index("pix")
    y = lax.axis_index("ray")
    x, c = pix // 2, lax.rem(pix, 2)
    xr, xl, xo = lax.rem(x + 1, n_x), lax.rem(x + n_x - 1, n_x), lax.rem(x + 2, n_x)
    yr, yl, yo = lax.rem(y + 1, n_y), lax.rem(y + n_y - 1, n_y), lax.rem(y + 2, n_y)
    right, left, sib = {"pix": xr * 2 + c}, {"pix": xl * 2 + c}, {"pix": x * 2 + 1 - c}
    up, down = {"ray": yr}, {"ray": yl}
    mine, theirs = c * n_x, (1 - c) * n_x
    k_chunks = range(len(CHUNKS))

    names = {}

    def tx(name, k, src, dst, dev):
        slot = names.setdefault((name, k), len(names))
        return pltpu.make_async_remote_copy(
            src_ref=src, dst_ref=dst, send_sem=send.at[slot], recv_sem=recv.at[slot],
            device_id=dev, device_id_type=MESH)

    def rows(k):
        o, n, _ = CHUNKS[k]
        return pl.ds(o, n)

    def h0(k):
        o, _, n0 = CHUNKS[k]
        return pl.ds(o, n0)

    def h1(k):
        o, n, n0 = CHUNKS[k]
        return pl.ds(o + n0, n - n0)

    def t_p(k, d):
        return tx("p", (k, d), ps.at[d, rows(k)], pd.at[d, rows(k)], sib)

    def t_x1r(k):
        return tx("x1r", k, ss.at[xo, h1(k)], q.at[h1(k)], right)

    def t_x1l(k):
        return tx("x1l", k, ss.at[xo, h0(k)], q.at[h0(k)], left)

    def t_xdr(k):
        return tx("xdr", k, ss.at[xr, h0(k)], fl.at[h0(k)], right)

    def t_xdl(k):
        return tx("xdl", k, ss.at[xl, h1(k)], fr.at[h1(k)], left)

    def t_x2r(k):
        return tx("x2r", k, ss.at[xr, h1(k)], fl.at[h1(k)], right)

    def t_x2l(k):
        return tx("x2l", k, ss.at[xl, h0(k)], fr.at[h0(k)], left)

    def gather(name, k, buf, sel, dev):
        return tx(name, k, buf.at[sel], buf.at[sel], dev)

    def t_g(k, buf=None, tag="g"):
        buf = rall if buf is None else buf
        return Lazy({
            "r": lambda: gather(tag + "r", k, buf, (mine + x, rows(k)), right),
            "l": lambda: gather(tag + "l", k, buf, (mine + x, rows(k)), left),
            "s": lambda: gather(tag + "s", k, buf, (mine + x, rows(k)), sib),
            "hr": lambda: gather(tag + "hr", k, buf, (mine + xl, h1(k)), right),
            "hl": lambda: gather(tag + "hl", k, buf, (mine + xr, h0(k)), left),
            "sl": lambda: gather(tag + "sl", k, buf, (mine + xl, rows(k)), sib),
            "sr": lambda: gather(tag + "sr", k, buf, (mine + xr, rows(k)), sib),
            "so": lambda: gather(tag + "so", k, buf, (mine + xo, rows(k)), sib),
        })

    half = cy // 2
    yh0, yh1 = pl.ds(0, half), pl.ds(half, cy - half)
    lane0 = (width // 256 + (1 if width % 256 else 0)) * 128
    lane_a, lane_b = pl.ds(0, lane0), pl.ds(lane0, width - lane0)

    t_y1r = lambda: tx("y1r", 0, gt.at[yo, yh1], qy.at[yh1], up)
    t_y1l = lambda: tx("y1l", 0, gt.at[yo, yh0], qy.at[yh0], down)
    t_ydr = lambda: tx("ydr", 0, gt.at[yr, yh0], fyl.at[yh0], up)
    t_ydl = lambda: tx("ydl", 0, gt.at[yl, yh1], fyr.at[yh1], down)
    t_y2r = lambda: tx("y2r", 0, gt.at[yr, yh1], fyl.at[yh1], up)
    t_y2l = lambda: tx("y2l", 0, gt.at[yl, yh0], fyr.at[yh0], down)

    def t_z(buf, tag):
        every = pl.ds(0, cy)
        return Lazy({
            "r": lambda: gather(tag + "r", 0, buf, (y,), up),
            "l": lambda: gather(tag + "l", 0, buf, (y,), down),
            "hr": lambda: gather(tag + "hr", 0, buf, (yl, every, lane_b), up),
            "hl": lambda: gather(tag + "hl", 0, buf, (yr, every, lane_a), down),
        })

    barrier = pltpu.get_barrier_semaphore()
    for j in range(1, ring_x):
        pl.semaphore_signal(barrier, inc=1, device_id={"pix": lax.rem(pix + j, ring_x)}, device_id_type=MESH)
    for j in range(1, ring_y):
        pl.semaphore_signal(barrier, inc=1, device_id={"ray": lax.rem(y + j, ring_y)}, device_id_type=MESH)

    def load_a(o, k):
        return pltpu.make_async_copy(a_hbm.at[o, rows(k)], a_v.at[o, rows(k)], a_sem.at[k, o])

    def start_a(k, base):
        def one(d, _):
            load_a(base + d, k).start()
            return 0
        lax.fori_loop(0, n_x, one, 0)

    for k in k_chunks:
        start_a(k, theirs)
        start_a(k, mine)
    load_b = pltpu.make_async_copy(b_hbm.at[mine + x], b_v, b_sem)
    load_b.start()

    xn[...] = x_in[...].astype(BF16)
    xf[...] = x_in[...].T.reshape(xf.shape)
    xs[...] = xf[y]
    sqv[...] = jnp.zeros_like(sqv)
    load_b.wait()
    pl.semaphore_wait(barrier, ring_x - 1 + ring_y - 1)

    def project(s, k, base, dst, first):
        def one(d, _):
            if first:
                load_a(base + d, k).wait()
            dst[d, rows(k)] = jnp.dot(a_v[base + d, rows(k)], xn[...], preferred_element_type=F32)
            return 0
        lax.fori_loop(0, n_x, one, 0)

    def sweep(s, first, last):
        def F_sib(k):
            project(s, k, theirs, ps, first)
            for d in range(n_x):
                t_p(k, d).start()

        def F_own(k):
            project(s, k, mine, ss, first)

        def D(k):
            for d in range(n_x):
                t_p(k, d).wait_recv()
            for d in range(n_x):
                ss[d, rows(k)] = ss[d, rows(k)] + pd[d, rows(k)]
            t_x1r(k).start()
            t_x1l(k).start()
            t_xdr(k).start()
            t_xdl(k).start()

        def L(k):
            t_x1r(k).wait_recv()
            ss[xr, h1(k)] = ss[xr, h1(k)] + q[h1(k)]
            t_x2r(k).start()
            t_x1l(k).wait_recv()
            ss[xl, h0(k)] = ss[xl, h0(k)] + q[h0(k)]
            t_x2l(k).start()

        def O(k):
            t_xdr(k).wait_recv()
            t_xdl(k).wait_recv()
            t_x2r(k).wait_recv()
            t_x2l(k).wait_recv()
            total = ss[x, rows(k)] + fl[rows(k)] + fr[rows(k)]
            r = rinv[rows(k)] * (b_v[rows(k)] - total)
            rall[mine + x, rows(k)] = r.astype(BF16)
            part = jnp.sum(r * r, axis=0, keepdims=True)
            if k == 0:
                sqv[pl.ds(s, 1)] = part
            else:
                sqv[pl.ds(s, 1)] = sqv[pl.ds(s, 1)] + part
            if last:
                rf[mine + x, rows(k)] = r
            t = t_g(k)
            t["r"].start()
            t["l"].start()
            t["s"].start()

        def A(k, buf=None, tag="g"):
            t = t_g(k, buf, tag)
            t["r"].wait_recv()
            t["hr"].start()
            t["sl"].start()
            t["l"].wait_recv()
            t["hl"].start()
            t["sr"].start()

        def A2(k, buf=None, tag="g"):
            t = t_g(k, buf, tag)
            t["hr"].wait_recv()
            t["hl"].wait_recv()
            t["so"].start()

        def back(o, k, init=False):
            part = lax.dot_general(rall[o, rows(k)], a_v[o, rows(k)], (((0,), (0,)), ((), ())),
                                   preferred_element_type=F32).reshape(gt.shape)
            if init:
                gt[...] = part
            else:
                gt[...] = gt[...] + part

        def B_own(k):
            back(mine + x, k, init=(k == 0))

        def B_near(k):
            back(mine + xl, k)
            back(mine + xr, k)

        def B_far(k):
            t = t_g(k)
            t["s"].wait_recv()
            back(theirs + x, k)
            t["sl"].wait_recv()
            back(theirs + xl, k)
            t["sr"].wait_recv()
            back(theirs + xr, k)
            back(mine + xo, k)
            t["so"].wait_recv()
            back(theirs + xo, k)

        F_sib(0); F_own(0); F_sib(1); D(0); F_own(1); F_sib(2); D(1); L(0); F_own(2); D(2); L(1)
        O(0); B_own(0); L(2); A(0); O(1); B_near(0); A2(0); A(1); O(2); B_far(0)
        B_own(1); B_near(1); A2(1); A(2); B_own(2); B_far(1); A2(2); B_near(2); B_far(2)

        t_y1r().start()
        t_y1l().start()
        t_ydr().start()
        t_ydl().start()
        if last:
            for k in k_chunks:
                t = t_g(k, rf, "f")
                t["r"].start()
                t["l"].start()
                t["s"].start()
        t_y1r().wait_recv()
        gt[yr, yh1] = gt[yr, yh1] + qy[yh1]
        t_y2r().start()
        t_y1l().wait_recv()
        gt[yl, yh0] = gt[yl, yh0] + qy[yh0]
        t_y2l().start()
        t_ydr().wait_recv()
        t_ydl().wait_recv()
        t_y2r().wait_recv()
        t_y2l().wait_recv()
        xs[...] = xs[...] + lam[0] * cinv[...] * (gt[y] + fyl[...] + fyr[...])
        if last:
            buf, tag = xf, "w"
            xf[y] = xs[...]
        else:
            buf, tag = xb, "z"
            xb[y] = xs[...].astype(BF16)
        z = t_z(buf, tag)
        z["r"].start()
        z["l"].start()
        if last:
            sq_sends = squares()
            for k in k_chunks:
                A(k, rf, "f")
        z["r"].wait_recv()
        z["hr"].start()
        z["l"].wait_recv()
        z["hl"].start()
        if last:
            for k in k_chunks:
                A2(k, rf, "f")
        z["hr"].wait_recv()
        z["hl"].wait_recv()
        if last:
            x_out[...] = xf[...].reshape(cy * n_y, width).T
            for k in k_chunks:
                t = t_g(k, rf, "f")
                for key in ("s", "sl", "sr", "so"):
                    t[key].wait_recv()
            out = pltpu.make_async_copy(rf, r_out, o_sem)
            out.start()
            out.wait()
        else:
            xn[...] = xb[...].reshape(cy * n_y, width).T

        for k in k_chunks:
            for d in range(n_x):
                t_p(k, d).wait_send()
            for t in (t_x1r, t_x1l, t_xdr, t_xdl, t_x2r, t_x2l):
                t(k).wait_send()
            for t in t_g(k).values():
                t.wait_send()
            if last:
                for t in t_g(k, rf, "f").values():
                    t.wait_send()
        for t in (t_y1r, t_y1l, t_ydr, t_ydl, t_y2r, t_y2l):
            t().wait_send()
        for t in z.values():
            t.wait_send()
        if last:
            for t in sq_sends:
                t.wait_send()

    def squares():
        sends = []
        sqr[pix] = sqv[...]
        for j in range(1, ring_x):
            t = tx("qx", j, sqr.at[pix], sqr.at[pix], {"pix": lax.rem(pix + j, ring_x)})
            t.start()
            sends.append(t)
        for t in sends:
            t.wait_recv()
        total = sqr[0]
        for j in range(1, ring_x):
            total = total + sqr[j]
        sqc[y] = total
        more = []
        for j in range(1, ring_y):
            t = tx("qy", j, sqc.at[y], sqc.at[y], {"ray": lax.rem(y + j, ring_y)})
            t.start()
            more.append(t)
        for t in more:
            t.wait_recv()
        total = sqc[0]
        for j in range(1, ring_y):
            total = total + sqc[j]
        s_out[...] = (total / ray_total)[:SWEEPS]
        return sends + more

    sweep(0, True, False)

    def body(s, _):
        sweep(s, False, False)
        return 0

    lax.fori_loop(1, SWEEPS - 1, body, 0)
    sweep(SWEEPS - 1, False, True)


def solution(mesh):
    ring_x, ring_y = mesh.shape["pix"], mesh.shape["ray"]

    def local_sweeps(a_blk, x_loc, sino_loc, row_inv, col_inv, relaxation):
        rays, width = a_blk.shape
        cols = x_loc.shape[1]
        rp, cy, n_x = rays // ring_x, cols // ring_y, ring_x // 2
        pix = lax.axis_index("pix")
        owner = lax.rem(pix, 2) * n_x + pix // 2
        rinv = jnp.broadcast_to(lax.dynamic_slice(row_inv, (owner * rp,), (rp,))[:, None], (rp, cols))
        cinv = jnp.broadcast_to(col_inv[None, :], (cy, width))
        vmem = pl.BlockSpec(memory_space=pltpu.VMEM)
        hbm = pl.BlockSpec(memory_space=pl.ANY)
        smem = pl.BlockSpec(memory_space=pltpu.SMEM)
        x_fin, resid, sq = pl.pallas_call(
            functools.partial(_kernel, ring_x, ring_y, rays * ring_y),
            out_shape=(
                jax.ShapeDtypeStruct((width, cols), F32),
                jax.ShapeDtypeStruct((ring_x, rp, cols), F32),
                jax.ShapeDtypeStruct((SWEEPS, cols), F32),
            ),
            in_specs=[hbm, vmem, hbm, vmem, vmem, smem],
            out_specs=(vmem, hbm, vmem),
            scratch_shapes=[
                pltpu.VMEM((ring_x, rp, width), BF16),
                pltpu.VMEM((rp, cols), F32),
                pltpu.VMEM((n_x, rp, cols), F32),
                pltpu.VMEM((n_x, rp, cols), F32),
                pltpu.VMEM((n_x, rp, cols), F32),
                pltpu.VMEM((rp, cols), F32),
                pltpu.VMEM((rp, cols), F32),
                pltpu.VMEM((rp, cols), F32),
                pltpu.VMEM((ring_x, rp, cols), BF16),
                pltpu.VMEM((ring_x, rp, cols), F32),
                pltpu.VMEM((ring_y, cy, width), F32),
                pltpu.VMEM((cy, width), F32),
                pltpu.VMEM((cy, width), F32),
                pltpu.VMEM((cy, width), F32),
                pltpu.VMEM((cy, width), F32),
                pltpu.VMEM((ring_y, cy, width), BF16),
                pltpu.VMEM((ring_y, cy, width), F32),
                pltpu.VMEM((width, cols), BF16),
                pltpu.VMEM((8, cols), F32),
                pltpu.VMEM((ring_x, 8, cols), F32),
                pltpu.VMEM((ring_y, 8, cols), F32),
                pltpu.SemaphoreType.DMA((len(CHUNKS), ring_x)),
                pltpu.SemaphoreType.DMA,
                pltpu.SemaphoreType.DMA,
                pltpu.SemaphoreType.DMA((128,)),
                pltpu.SemaphoreType.DMA((128,)),
            ],
            compiler_params=pltpu.CompilerParams(
                collective_id=0, has_side_effects=True, vmem_limit_bytes=60 * 1024 * 1024),
        )(a_blk.reshape(ring_x, rp, width), x_loc, sino_loc.reshape(ring_x, rp, cols), rinv, cinv, relaxation.reshape(1))
        return x_fin, resid.reshape(rays, cols), sq

    return jax.shard_map(
        local_sweeps,
        mesh=mesh,
        in_specs=(P("ray", "pix"), P("pix", "part"), P("ray", "part"), P("ray"), P("pix"), P()),
        out_specs=(P("pix", "part"), P("ray", "part"), P(None, "part")),
        check_vma=False,
    )
```

```python
import functools

import jax
import jax.numpy as jnp
from jax import lax
from jax.experimental import pallas as pl
from jax.experimental.pallas import tpu as pltpu
from jax.sharding import PartitionSpec as P

SWEEPS = 6
GROUPS = 2
MESH = pl.DeviceIdType.MESH
F32 = jnp.float32
BF16 = jnp.bfloat16

CHUNKS = ((0, 128), (128, 128), (256, 112))


def _kernel(ring_x, ring_y, ray_total, a_hbm, x_in, b_hbm, rinv_in, cinv, lam, x_out, r_out, s_out,
            a_v, b_v, rinv, bp, ps, pd, ss, fin, rall, rf, gt, fy, xs, xb, xf, xn, sqv, sqr, sqc,
            a_sem, b_sem, x_sem, r_sem, send, recv):
    own_rows = b_hbm.shape[1]
    packed = ss.shape[2]
    lanes = ss.shape[3]
    half = lanes // GROUPS
    cy, width = gt.shape[2], gt.shape[3]
    n_x, n_y = ring_x // 2, ring_y
    pix = lax.axis_index("pix")
    y = lax.axis_index("ray")
    x, c = pix // 2, lax.rem(pix, 2)
    sib = {"pix": x * 2 + 1 - c}
    mine, theirs = c * n_x, (1 - c) * n_x
    chunks = range(len(CHUNKS))
    others_x, others_y = range(1, n_x), range(1, n_y)

    def at_x(j):
        return lax.rem(x + j, n_x)

    def at_y(j):
        return lax.rem(y + j, n_y)

    def core_at(j):
        return {"pix": at_x(j) * 2 + c}

    names = {}

    def tx(name, src, dst, dev):
        slot = names.setdefault(name, len(names))
        return pltpu.make_async_remote_copy(
            src_ref=src, dst_ref=dst, send_sem=send.at[slot], recv_sem=recv.at[slot],
            device_id=dev, device_id_type=MESH)

    def rows(k):
        return pl.ds(*CHUNKS[k])

    def low_rows(k):
        return pl.ds(packed + CHUNKS[k][0], CHUNKS[k][1])

    def t_p(g, k):
        return tx(("p", g, k), ps.at[g, :, rows(k)], pd.at[g, :, rows(k)], sib)

    def t_x(g, k, j):
        return tx(("x", g, k, j), ss.at[g, at_x(j), rows(k)], fin.at[g, j - 1, rows(k)], core_at(j))

    def t_r(g, k, j):
        ref = rall.at[g, mine + x, rows(k)]
        return tx(("r", g, k, j), ref, ref, core_at(j))

    def t_s(g, k, j):
        ref = rall.at[g, mine + at_x(n_x - j), rows(k)]
        return tx(("s", g, k, j), ref, ref, sib)

    def t_rf(g, j):
        ref = rf.at[g, mine + x]
        return tx(("rf", g, j), ref, ref, core_at(j))

    def t_sf(g, j):
        ref = rf.at[g, mine + at_x(n_x - j)]
        return tx(("sf", g, j), ref, ref, sib)

    def t_y(g, j):
        return tx(("y", g, j), gt.at[g, at_y(j)], fy.at[g, j - 1], {"ray": at_y(j)})

    def t_z(g, j):
        return tx(("z", g, j), xb.at[g, y], xb.at[g, y], {"ray": at_y(j)})

    def t_w(g, j):
        return tx(("w", g, j), xf.at[g, y], xf.at[g, y], {"ray": at_y(j)})

    def t_qx(j):
        return tx(("qx", j), sqr.at[pix], sqr.at[pix], {"pix": lax.rem(pix + j, ring_x)})

    def t_qy(j):
        return tx(("qy", j), sqc.at[y], sqc.at[y], {"ray": at_y(j)})

    barrier = pltpu.get_barrier_semaphore()
    for j in range(1, ring_x):
        pl.semaphore_signal(barrier, inc=1, device_id={"pix": lax.rem(pix + j, ring_x)}, device_id_type=MESH)
    for j in others_y:
        pl.semaphore_signal(barrier, inc=1, device_id={"ray": at_y(j)}, device_id_type=MESH)

    def load_a(part, k):
        base = theirs if part == 0 else mine
        low = min(CHUNKS[k][1], own_rows - packed - CHUNKS[k][0])
        owners = pl.ds(base, n_x)
        return [pltpu.make_async_copy(a_hbm.at[owners, sl], a_v.at[owners, sl], a_sem.at[part, k, i])
                for i, sl in enumerate((rows(k), pl.ds(packed + CHUNKS[k][0], low)))]

    load_b = pltpu.make_async_copy(b_hbm.at[mine + x], b_v.at[pl.ds(0, own_rows)], b_sem)
    load_b.start()
    for k in chunks:
        for part in (0, 1):
            for t in load_a(part, k):
                t.start()
    pad = 2 * packed - own_rows
    a_v[:, pl.ds(own_rows, pad)] = jnp.zeros((ring_x, pad, width), BF16)
    b_v[pl.ds(own_rows, pad)] = jnp.zeros((pad, lanes), F32)
    sqv[...] = jnp.zeros_like(sqv)

    def first_half(shape):
        return lax.broadcasted_iota(jnp.int32, shape, len(shape) - 1) < half

    def swap(v):
        return pltpu.roll(v, half, 1)

    image = x_in[...]
    keep = first_half(image.shape)
    first = jnp.where(keep, image, 0.0)
    second = jnp.where(keep, 0.0, image)
    xn[0, 0] = first.astype(BF16)
    xn[0, 1] = swap(first).astype(BF16)
    xn[1, 0] = swap(second).astype(BF16)
    xn[1, 1] = second.astype(BF16)
    xf[...] = image.T.reshape(xf.shape)
    for g in range(GROUPS):
        xs[g] = xf[g, y]
    weights = rinv_in[pl.ds(mine + x, 1)]
    weights = jnp.broadcast_to(weights, (lanes, weights.shape[1])).T
    rinv[...] = jnp.where(first_half((packed, lanes)), weights[:packed], weights[packed:2 * packed])
    load_b.wait()
    top, low = b_v[pl.ds(0, packed)], b_v[pl.ds(packed, packed)]
    keep = first_half(top.shape)
    bp[0] = jnp.where(keep, top, swap(low))
    bp[1] = jnp.where(keep, swap(top), low)
    pl.semaphore_wait(barrier, ring_x - 1 + ring_y - 1)

    def block(part, k):
        base = theirs if part == 0 else mine
        n = CHUNKS[k][1]
        return (a_v[pl.ds(base, n_x), rows(k)].reshape(n_x * n, width),
                a_v[pl.ds(base, n_x), low_rows(k)].reshape(n_x * n, width))

    def F(g, s, part, k):
        if g == 0:
            @pl.when(s == 0)
            def _():
                for t in load_a(part, k):
                    t.wait()
        upper, lower = block(part, k)
        out = (jnp.dot(upper, xn[g, 0], preferred_element_type=F32)
               + jnp.dot(lower, xn[g, 1], preferred_element_type=F32))
        dst = ps if part == 0 else ss
        dst[g, :, rows(k)] = out.reshape(n_x, CHUNKS[k][1], lanes)
        if part == 0:
            t_p(g, k).start()

    def D(g, s, k):
        t_p(g, k).wait_recv()
        ss[g, :, rows(k)] = ss[g, :, rows(k)] + pd[g, :, rows(k)]
        for j in others_x:
            t_x(g, k, j).start()

    def O(g, s, k):
        for j in others_x:
            t_x(g, k, j).wait_recv()
        total = ss[g, x, rows(k)]
        for j in others_x:
            total = total + fin[g, j - 1, rows(k)]
        r = rinv[rows(k)] * (bp[g, rows(k)] - total)
        rall[g, mine + x, rows(k)] = r.astype(BF16)
        rf[g, mine + x, rows(k)] = r
        for j in others_x:
            t_r(g, k, j).start()
        t_s(g, k, 0).start()
        part = jnp.sum(r * r, axis=0, keepdims=True)
        sqv[g, pl.ds(s, 1)] = sqv[g, pl.ds(s, 1)] + part

    def A(g, s, k):
        for j in others_x:
            t_r(g, k, j).wait_recv()
            t_s(g, k, j).start()

    def B(g, s, part, k):
        if part == 0:
            for j in range(n_x):
                t_s(g, k, j).wait_recv()
        upper, lower = block(part, k)
        base = theirs if part == 0 else mine
        rt = rall[g, pl.ds(base, n_x), rows(k)].reshape(n_x * CHUNKS[k][1], lanes).T
        out = (jnp.dot(rt[:half], upper, preferred_element_type=F32)
               + jnp.dot(rt[half:], lower, preferred_element_type=F32)).reshape(n_y, cy, width)
        if part == 1 and k == 0:
            gt[g] = out
        else:
            gt[g] = gt[g] + out

    def Y0(g, s):
        for j in others_y:
            t_y(g, j).start()

        @pl.when(s == SWEEPS - 1)
        def _():
            for j in others_x:
                t_rf(g, j).start()
            t_sf(g, 0).start()

    def Y1(g, s):
        for j in others_y:
            t_y(g, j).wait_recv()
        total = gt[g, y]
        for j in others_y:
            total = total + fy[g, j - 1]
        image = xs[g] + lam[0] * cinv[...] * total
        xs[g] = image

        @pl.when(s < SWEEPS - 1)
        def _():
            xb[g, y] = image.astype(BF16)
            for j in others_y:
                t_z(g, j).start()

        @pl.when(s == SWEEPS - 1)
        def _():
            xf[g, y] = image
            for j in others_y:
                t_w(g, j).start()

    def Y2(g, s):
        @pl.when(s < SWEEPS - 1)
        def _():
            for j in others_y:
                t_z(g, j).wait_recv()
            image = xb[g].reshape(n_y * cy, width)
            none = jnp.zeros_like(image)
            xn[g, 0] = jnp.concatenate([image, none], axis=0).T
            xn[g, 1] = jnp.concatenate([none, image], axis=0).T
            for j in others_y:
                t_z(g, j).wait_send()

        @pl.when(s == SWEEPS - 1)
        def _():
            for j in others_x:
                t_rf(g, j).wait_recv()
                t_sf(g, j).start()
            for j in others_y:
                t_w(g, j).wait_recv()
                t_w(g, j).wait_send()

        for k in chunks:
            t_p(g, k).wait_send()
            for j in others_x:
                t_x(g, k, j).wait_send()
                t_r(g, k, j).wait_send()
            for j in range(n_x):
                t_s(g, k, j).wait_send()
        for j in others_y:
            t_y(g, j).wait_send()

    def Q0():
        sqr[pix] = sqv[...]
        for j in range(1, ring_x):
            t_qx(j).start()

    def Q1():
        for j in range(1, ring_x):
            t_qx(j).wait_recv()
        total = sqr[0]
        for j in range(1, ring_x):
            total = total + sqr[j]
        sqc[y] = total
        for j in others_y:
            t_qy(j).start()

    ORDER = (
        "aF00", "bA1", "aF10", "bB11", "bA2", "bB00", "aD0", "bB01",
        "aF01", "bB02", "bB12", "bY0", "aF11", "aD1", "aF02", "aF12",
        "aD2", "aO0", "bY1", "aO1", "aO2", "aA0", "aB10", "bY2",
    )
    TABLE = {"D": D, "O": O, "A": A}

    def run(op, g, s):
        if op[0] == "F":
            F(g, s, int(op[1]), int(op[2]))
        elif op[0] == "B":
            B(g, s, int(op[1]), int(op[2]))
        elif op[0] == "Y":
            (Y0, Y1, Y2)[int(op[1])](g, s)
        else:
            TABLE[op[0]](g, s, int(op[1]))

    def half_sweep(a, sa, b, sb, guard):
        for op in ORDER:
            g, s = (a, sa) if op[0] == "a" else (b, sb)
            if guard:
                pl.when(sa < SWEEPS if op[0] == "a" else sb >= 0)(functools.partial(run, op[1:], g, s))
                if op in ("bY0", "bY1"):
                    pl.when(sb == SWEEPS - 1)(Q0 if op == "bY0" else Q1)
            else:
                run(op[1:], g, s)

    def body(s, _):
        half_sweep(0, s, 1, s - 1, True)

        @pl.when(s < SWEEPS)
        def _():
            half_sweep(1, s, 0, s, False)
        return 0

    lax.fori_loop(0, SWEEPS + 1, body, 0)

    put_x = pltpu.make_async_copy(xf, x_out, x_sem)
    put_x.start()
    for g in range(GROUPS):
        for j in range(n_x):
            t_sf(g, j).wait_recv()
    put_r = pltpu.make_async_copy(rf, r_out, r_sem)
    put_r.start()
    for j in others_y:
        t_qy(j).wait_recv()
    total = sqc[0]
    for j in others_y:
        total = total + sqc[j]
    s_out[...] = total / ray_total
    put_x.wait()
    put_r.wait()
    for g in range(GROUPS):
        for j in others_x:
            t_rf(g, j).wait_send()
        for j in range(n_x):
            t_sf(g, j).wait_send()
    for j in range(1, ring_x):
        t_qx(j).wait_send()
    for j in others_y:
        t_qy(j).wait_send()


def _finish(rf, xf, sq, x_out, r_out, s_out):
    packed, lanes = rf.shape[2], rf.shape[3]
    left = lax.broadcasted_iota(jnp.int32, (packed, lanes), 1) < lanes // GROUPS

    def swap(v):
        return pltpu.roll(v, lanes // GROUPS, 1)

    for i in range(r_out.shape[0]):
        one, two = rf[0, i], rf[1, i]
        r_out[i, pl.ds(0, packed)] = jnp.where(left, one, swap(two))
        rest = r_out.shape[1] - packed
        r_out[i, pl.ds(packed, rest)] = jnp.where(left, swap(one), two)[:rest]

    @pl.when(pl.program_id(0) == 0)
    def _():
        x_out[...] = xf[...].reshape(lanes, x_out.shape[0]).T
        both = [sq[g] + swap(sq[g]) for g in range(GROUPS)]
        s_out[...] = jnp.where(left[:8], both[0], both[1])[:SWEEPS]


def solution(mesh):
    ring_x, ring_y = mesh.shape["pix"], mesh.shape["ray"]

    def local_sweeps(a_blk, x_loc, sino_loc, row_inv, col_inv, relaxation):
        rays, width = a_blk.shape
        cols = x_loc.shape[1]
        rp, cy, n_x = rays // ring_x, cols // ring_y // GROUPS, ring_x // 2
        packed = sum(n for _, n in CHUNKS)
        lane_rows = -(-2 * packed // 128) * 128
        rinv = jnp.pad(row_inv.reshape(ring_x, rp), ((0, 0), (0, lane_rows - rp)))
        cinv = col_inv.reshape(1, width)
        vmem = pl.BlockSpec(memory_space=pltpu.VMEM)
        hbm = pl.BlockSpec(memory_space=pl.ANY)
        smem = pl.BlockSpec(memory_space=pltpu.SMEM)
        x_part, r_part, s_part = pl.pallas_call(
            functools.partial(_kernel, ring_x, ring_y, rays * ring_y),
            out_shape=(
                jax.ShapeDtypeStruct((GROUPS, ring_y, cy, width), F32),
                jax.ShapeDtypeStruct((GROUPS, ring_x, packed, cols), F32),
                jax.ShapeDtypeStruct((GROUPS, 8, cols), F32),
            ),
            in_specs=[hbm, vmem, hbm, vmem, vmem, smem],
            out_specs=(hbm, hbm, vmem),
            scratch_shapes=[
                pltpu.VMEM((ring_x, 2 * packed, width), BF16),
                pltpu.VMEM((2 * packed, cols), F32),
                pltpu.VMEM((packed, cols), F32),
                pltpu.VMEM((GROUPS, packed, cols), F32),
                pltpu.VMEM((GROUPS, n_x, packed, cols), F32),
                pltpu.VMEM((GROUPS, n_x, packed, cols), F32),
                pltpu.VMEM((GROUPS, n_x, packed, cols), F32),
                pltpu.VMEM((GROUPS, n_x - 1, packed, cols), F32),
                pltpu.VMEM((GROUPS, ring_x, packed, cols), BF16),
                pltpu.VMEM((GROUPS, ring_x, packed, cols), F32),
                pltpu.VMEM((GROUPS, ring_y, cy, width), F32),
                pltpu.VMEM((GROUPS, ring_y - 1, cy, width), F32),
                pltpu.VMEM((GROUPS, cy, width), F32),
                pltpu.VMEM((GROUPS, ring_y, cy, width), BF16),
                pltpu.VMEM((GROUPS, ring_y, cy, width), F32),
                pltpu.VMEM((GROUPS, 2, width, cols), BF16),
                pltpu.VMEM((GROUPS, 8, cols), F32),
                pltpu.VMEM((ring_x, GROUPS, 8, cols), F32),
                pltpu.VMEM((ring_y, GROUPS, 8, cols), F32),
                pltpu.SemaphoreType.DMA((2, len(CHUNKS), 2)),
                pltpu.SemaphoreType.DMA,
                pltpu.SemaphoreType.DMA,
                pltpu.SemaphoreType.DMA,
                pltpu.SemaphoreType.DMA((160,)),
                pltpu.SemaphoreType.DMA((160,)),
            ],
            compiler_params=pltpu.CompilerParams(
                collective_id=0, has_side_effects=True, vmem_limit_bytes=60 * 1024 * 1024),
        )(a_blk.reshape(ring_x, rp, width), x_loc, sino_loc.reshape(ring_x, rp, cols), rinv, cinv, relaxation.reshape(1))
        step = ring_x // 4
        x_fin, resid, sq = pl.pallas_call(
            _finish,
            grid=(ring_x // step,),
            out_shape=(
                jax.ShapeDtypeStruct((width, cols), F32),
                jax.ShapeDtypeStruct((ring_x, rp, cols), F32),
                jax.ShapeDtypeStruct((SWEEPS, cols), F32),
            ),
            in_specs=[
                pl.BlockSpec((GROUPS, step, packed, cols), lambda i: (0, i, 0, 0)),
                pl.BlockSpec((GROUPS, ring_y, cy, width), lambda i: (0, 0, 0, 0)),
                pl.BlockSpec((GROUPS, 8, cols), lambda i: (0, 0, 0)),
            ],
            out_specs=(
                pl.BlockSpec((width, cols), lambda i: (0, 0)),
                pl.BlockSpec((step, rp, cols), lambda i: (i, 0, 0)),
                pl.BlockSpec((SWEEPS, cols), lambda i: (0, 0)),
            ),
        )(r_part, x_part, s_part)
        return x_fin, resid.reshape(rays, cols), sq

    return jax.shard_map(
        local_sweeps,
        mesh=mesh,
        in_specs=(P("ray", "pix"), P("pix", "part"), P("ray", "part"), P("ray"), P("pix"), P()),
        out_specs=(P("pix", "part"), P("ray", "part"), P(None, "part")),
        check_vma=False,
    )
```

```python
import functools

import jax
import jax.numpy as jnp
from jax import lax
from jax.experimental import pallas as pl
from jax.experimental.pallas import tpu as pltpu
from jax.sharding import PartitionSpec as P

SWEEPS = 6
GROUPS = 2
MESH = pl.DeviceIdType.MESH
F32 = jnp.float32
BF16 = jnp.bfloat16

CHUNKS = ((0, 128), (128, 128), (256, 112))


def _kernel(ring_x, ring_y, ray_total, a_hbm, x_in, b_hbm, rinv_in, cinv_in, lam, x_out, r_out, s_out,
            a_v, b_v, line, rinv, cinv, bp, ps, pd, ss, fin, rall, rf, gt, fy, xs, xb, xf, xn, sqv, sqr, sqc,
            a_sem, b_sem, x_sem, r_sem, send, recv):
    own_rows = b_hbm.shape[1]
    packed = ss.shape[2]
    lanes = ss.shape[3]
    half = lanes // GROUPS
    cy, width = gt.shape[2], gt.shape[3]
    n_x, n_y = ring_x // 2, ring_y
    pix = lax.axis_index("pix")
    y = lax.axis_index("ray")
    x, c = pix // 2, lax.rem(pix, 2)
    sib = {"pix": x * 2 + 1 - c}
    mine, theirs = c * n_x, (1 - c) * n_x
    chunks = range(len(CHUNKS))
    others_x, others_y = range(1, n_x), range(1, n_y)
    far_first_x = sorted(others_x, key=lambda j: -min(j, n_x - j))
    far_first_y = sorted(others_y, key=lambda j: -min(j, n_y - j))
    near_first_x = sorted(others_x, key=lambda j: min(j, n_x - j))
    first_lanes = -(-width // 256) * 128
    parts_y = (pl.ds(0, first_lanes), pl.ds(first_lanes, width - first_lanes))

    def at_x(j):
        return lax.rem(x + j, n_x)

    def at_y(j):
        return lax.rem(y + j, n_y)

    def core_at(j):
        return {"pix": at_x(j) * 2 + c}

    names = {}

    def tx(name, src, dst, dev):
        slot = names.setdefault(name, len(names))
        return pltpu.make_async_remote_copy(
            src_ref=src, dst_ref=dst, send_sem=send.at[slot], recv_sem=recv.at[slot],
            device_id=dev, device_id_type=MESH)

    def rows(k):
        return pl.ds(*CHUNKS[k])

    def low_rows(k):
        return pl.ds(packed + CHUNKS[k][0], CHUNKS[k][1])

    def t_p(g, k):
        return tx(("p", g, k), ps.at[g, :, rows(k)], pd.at[g, :, rows(k)], sib)

    def t_x(g, k, j):
        return tx(("x", g, k, j), ss.at[g, at_x(j), rows(k)], fin.at[g, j - 1, rows(k)], core_at(j))

    def t_r(g, k, j):
        ref = rall.at[g, mine + x, rows(k)]
        return tx(("r", g, k, j), ref, ref, core_at(j))

    def t_s(g, k, j):
        ref = rall.at[g, mine + at_x(n_x - j), rows(k)]
        return tx(("s", g, k, j), ref, ref, sib)

    def t_rf(g, j):
        ref = rf.at[g, mine + x]
        return tx(("rf", g, j), ref, ref, core_at(j))

    def t_sf(g, j):
        ref = rf.at[g, mine + at_x(n_x - j)]
        return tx(("sf", g, j), ref, ref, sib)

    def t_y(g, i, j):
        return tx(("y", g, i, j), gt.at[g, at_y(j), :, parts_y[i]], fy.at[g, j - 1, :, parts_y[i]], {"ray": at_y(j)})

    def t_z(g, i, j):
        ref = xb.at[g, y, :, parts_y[i]]
        return tx(("z", g, i, j), ref, ref, {"ray": at_y(j)})

    def t_w(g, i, j):
        ref = xf.at[g, y, :, parts_y[i]]
        return tx(("w", g, i, j), ref, ref, {"ray": at_y(j)})

    def t_qx(j):
        return tx(("qx", j), sqr.at[pix], sqr.at[pix], {"pix": lax.rem(pix + j, ring_x)})

    def t_qy(j):
        return tx(("qy", j), sqc.at[y], sqc.at[y], {"ray": at_y(j)})

    barrier = pltpu.get_barrier_semaphore()
    for j in range(1, ring_x):
        pl.semaphore_signal(barrier, inc=1, device_id={"pix": lax.rem(pix + j, ring_x)}, device_id_type=MESH)
    for j in others_y:
        pl.semaphore_signal(barrier, inc=1, device_id={"ray": at_y(j)}, device_id_type=MESH)

    def load_a(part, k):
        base = theirs if part == 0 else mine
        low = min(CHUNKS[k][1], own_rows - packed - CHUNKS[k][0])
        owners = pl.ds(base, n_x)
        return [pltpu.make_async_copy(a_hbm.at[owners, sl], a_v.at[owners, sl], a_sem.at[part, k, i])
                for i, sl in enumerate((rows(k), pl.ds(packed + CHUNKS[k][0], low)))]

    load_b = pltpu.make_async_copy(b_hbm.at[mine + x], b_v.at[pl.ds(0, own_rows)], b_sem)
    load_b.start()
    for k in chunks:
        for part in (0, 1):
            for t in load_a(part, k):
                t.start()
    pad = 2 * packed - own_rows
    a_v[:, pl.ds(own_rows, pad)] = jnp.zeros((ring_x, pad, width), BF16)
    b_v[pl.ds(own_rows, pad)] = jnp.zeros((pad, lanes), F32)
    sqv[...] = jnp.zeros_like(sqv)

    def first_half(shape):
        return lax.broadcasted_iota(jnp.int32, shape, len(shape) - 1) < half

    def swap(v):
        return pltpu.roll(v, half, 1)

    image = x_in[...]
    keep = first_half(image.shape)
    first = jnp.where(keep, image, 0.0)
    second = jnp.where(keep, 0.0, image)
    xn[0, 0] = first.astype(BF16)
    xn[0, 1] = swap(first).astype(BF16)
    xn[1, 0] = swap(second).astype(BF16)
    xn[1, 1] = second.astype(BF16)
    xf[...] = image.T.reshape(xf.shape)
    for g in range(GROUPS):
        xs[g] = xf[g, y]
    start = (mine + x) * own_rows
    tile = rinv_in.shape[1]
    for i in range(line.shape[1] // tile):
        row = rinv_in[pl.ds(lax.rem(start // tile + i, rinv_in.shape[0]), 1)]
        line[:, pl.ds(i * tile, tile)] = jnp.broadcast_to(row, (8, tile))
    for i in range(cinv_in.shape[0]):
        cinv[:, pl.ds(i * tile, tile)] = jnp.broadcast_to(cinv_in[pl.ds(i, 1)], (cy, tile))
    weights = pltpu.roll(line[...], lax.rem(line.shape[1] - lax.rem(start, tile), line.shape[1]), 1)
    weights = jnp.broadcast_to(weights[:1], (lanes, line.shape[1])).T
    real = lax.broadcasted_iota(jnp.int32, (packed, lanes), 0) < own_rows - packed
    rinv[...] = jnp.where(first_half((packed, lanes)), weights[:packed],
                          jnp.where(real, weights[packed:2 * packed], 0.0))
    load_b.wait()
    top, low = b_v[pl.ds(0, packed)], b_v[pl.ds(packed, packed)]
    keep = first_half(top.shape)
    bp[0] = jnp.where(keep, top, swap(low))
    bp[1] = jnp.where(keep, swap(top), low)
    pl.semaphore_wait(barrier, ring_x - 1 + ring_y - 1)

    def block(part, k):
        base = theirs if part == 0 else mine
        n = CHUNKS[k][1]
        return (a_v[pl.ds(base, n_x), rows(k)].reshape(n_x * n, width),
                a_v[pl.ds(base, n_x), low_rows(k)].reshape(n_x * n, width))

    def F(g, s, part, k):
        if g == 0:
            @pl.when(s == 0)
            def _():
                for t in load_a(part, k):
                    t.wait()
        upper, lower = block(part, k)
        out = (jnp.dot(upper, xn[g, 0], preferred_element_type=F32)
               + jnp.dot(lower, xn[g, 1], preferred_element_type=F32))
        dst = ps if part == 0 else ss
        dst[g, :, rows(k)] = out.reshape(n_x, CHUNKS[k][1], lanes)
        if part == 0:
            t_p(g, k).start()

    def D(g, s, k):
        t_p(g, k).wait_recv()
        ss[g, :, rows(k)] = ss[g, :, rows(k)] + pd[g, :, rows(k)]
        for j in far_first_x:
            t_x(g, k, j).start()

    def O(g, s, k):
        for j in others_x:
            t_x(g, k, j).wait_recv()
        total = ss[g, x, rows(k)]
        for j in others_x:
            total = total + fin[g, j - 1, rows(k)]
        r = rinv[rows(k)] * (bp[g, rows(k)] - total)
        rall[g, mine + x, rows(k)] = r.astype(BF16)
        rf[g, mine + x, rows(k)] = r
        for j in far_first_x:
            t_r(g, k, j).start()
        t_s(g, k, 0).start()
        part = jnp.sum(r * r, axis=0, keepdims=True)
        sqv[g, pl.ds(s, 1)] = sqv[g, pl.ds(s, 1)] + part

    def A(g, s, k):
        for j in near_first_x:
            t_r(g, k, j).wait_recv()
            t_s(g, k, j).start()

    def B(g, s, part, k):
        if part == 0:
            for j in range(n_x):
                t_s(g, k, j).wait_recv()
        upper, lower = block(part, k)
        base = theirs if part == 0 else mine
        rt = rall[g, pl.ds(base, n_x), rows(k)].reshape(n_x * CHUNKS[k][1], lanes).T
        out = (jnp.dot(rt[:half], upper, preferred_element_type=F32)
               + jnp.dot(rt[half:], lower, preferred_element_type=F32)).reshape(n_y, cy, width)
        if part == 1 and k == 0:
            gt[g] = out
        else:
            gt[g] = gt[g] + out

    def Y0(g, s):
        for i in (0, 1):
            for j in far_first_y:
                t_y(g, i, j).start()

        @pl.when(s == SWEEPS - 1)
        def _():
            for j in far_first_x:
                t_rf(g, j).start()
            t_sf(g, 0).start()

    def update(g, s, i):
        for j in others_y:
            t_y(g, i, j).wait_recv()
        lanes_i = parts_y[i]
        total = gt[g, y, :, lanes_i]
        for j in others_y:
            total = total + fy[g, j - 1, :, lanes_i]
        image = xs[g, :, lanes_i] + lam[0] * cinv[:, lanes_i] * total
        xs[g, :, lanes_i] = image

        @pl.when(s < SWEEPS - 1)
        def _():
            xb[g, y, :, lanes_i] = image.astype(BF16)
            for j in far_first_y:
                t_z(g, i, j).start()

        @pl.when(s == SWEEPS - 1)
        def _():
            xf[g, y, :, lanes_i] = image
            for j in far_first_y:
                t_w(g, i, j).start()

    def Y1(g, s):
        update(g, s, 0)

    def Y3(g, s):
        update(g, s, 1)

    def Y2(g, s):
        @pl.when(s < SWEEPS - 1)
        def _():
            for i in (0, 1):
                for j in others_y:
                    t_z(g, i, j).wait_recv()
            image = xb[g].reshape(n_y * cy, width)
            both = jnp.concatenate([image, image], axis=0).T
            keep = first_half(both.shape)
            xn[g, 0] = jnp.where(keep, both, jnp.zeros_like(both))
            xn[g, 1] = jnp.where(keep, jnp.zeros_like(both), both)
            for i in (0, 1):
                for j in others_y:
                    t_z(g, i, j).wait_send()

        @pl.when(s == SWEEPS - 1)
        def _():
            for j in near_first_x:
                t_rf(g, j).wait_recv()
                t_sf(g, j).start()
            for i in (0, 1):
                for j in others_y:
                    t_w(g, i, j).wait_recv()
                    t_w(g, i, j).wait_send()

        for k in chunks:
            t_p(g, k).wait_send()
            for j in others_x:
                t_x(g, k, j).wait_send()
                t_r(g, k, j).wait_send()
            for j in range(n_x):
                t_s(g, k, j).wait_send()
        for i in (0, 1):
            for j in others_y:
                t_y(g, i, j).wait_send()

    def Q0():
        sqr[pix] = sqv[...]
        for j in range(1, ring_x):
            t_qx(j).start()

    def Q1():
        for j in range(1, ring_x):
            t_qx(j).wait_recv()
        total = sqr[0]
        for j in range(1, ring_x):
            total = total + sqr[j]
        sqc[y] = total
        for j in others_y:
            t_qy(j).start()

    ORDER = (
        "aF02", "bA0", "aF00", "bA2", "aF10", "bB10", "bB12", "aD0",
        "bA1", "bB00", "bB11", "bB02", "bB01", "bY0", "aF12", "aD2",
        "aF01", "aF11", "aD1", "aO0", "bY1", "bY3", "aO2", "aO1",
        "bY2",
    )
    TABLE = {"D": D, "O": O, "A": A}

    def run(op, g, s):
        if op[0] == "F":
            F(g, s, int(op[1]), int(op[2]))
        elif op[0] == "B":
            B(g, s, int(op[1]), int(op[2]))
        elif op[0] == "Y":
            (Y0, Y1, Y2, Y3)[int(op[1])](g, s)
        else:
            TABLE[op[0]](g, s, int(op[1]))

    def half_sweep(a, sa, b, sb, guard):
        for op in ORDER:
            g, s = (a, sa) if op[0] == "a" else (b, sb)
            if guard:
                pl.when(sa < SWEEPS if op[0] == "a" else sb >= 0)(functools.partial(run, op[1:], g, s))
                if op in ("bY0", "bY1"):
                    pl.when(sb == SWEEPS - 1)(Q0 if op == "bY0" else Q1)
            else:
                run(op[1:], g, s)

    def body(s, _):
        half_sweep(0, s, 1, s - 1, True)

        @pl.when(s < SWEEPS)
        def _():
            half_sweep(1, s, 0, s, False)
        return 0

    lax.fori_loop(0, SWEEPS + 1, body, 0)

    put_x = pltpu.make_async_copy(xf, x_out, x_sem)
    put_x.start()
    for g in range(GROUPS):
        for j in range(n_x):
            t_sf(g, j).wait_recv()
    put_r = pltpu.make_async_copy(rf, r_out, r_sem)
    put_r.start()
    for j in others_y:
        t_qy(j).wait_recv()
    total = sqc[0]
    for j in others_y:
        total = total + sqc[j]
    s_out[...] = total / ray_total
    put_x.wait()
    put_r.wait()
    for g in range(GROUPS):
        for j in others_x:
            t_rf(g, j).wait_send()
        for j in range(n_x):
            t_sf(g, j).wait_send()
    for j in range(1, ring_x):
        t_qx(j).wait_send()
    for j in others_y:
        t_qy(j).wait_send()


def _finish(rf, xf, sq, x_out, r_out, s_out):
    packed, lanes = rf.shape[2], rf.shape[3]
    left = lax.broadcasted_iota(jnp.int32, (packed, lanes), 1) < lanes // GROUPS

    def swap(v):
        return pltpu.roll(v, lanes // GROUPS, 1)

    for i in range(r_out.shape[0]):
        one, two = rf[0, i], rf[1, i]
        r_out[i, pl.ds(0, packed)] = jnp.where(left, one, swap(two))
        rest = r_out.shape[1] - packed
        r_out[i, pl.ds(packed, rest)] = jnp.where(left, swap(one), two)[:rest]

    @pl.when(pl.program_id(0) == 1)
    def _():
        x_out[...] = xf[...].reshape(lanes, x_out.shape[0]).T
        both = [sq[g] + swap(sq[g]) for g in range(GROUPS)]
        s_out[...] = jnp.where(left[:8], both[0], both[1])[:SWEEPS]


def solution(mesh):
    ring_x, ring_y = mesh.shape["pix"], mesh.shape["ray"]

    def local_sweeps(a_blk, x_loc, sino_loc, row_inv, col_inv, relaxation):
        rays, width = a_blk.shape
        cols = x_loc.shape[1]
        rp, cy, n_x = rays // ring_x, cols // ring_y // GROUPS, ring_x // 2
        packed = sum(n for _, n in CHUNKS)
        rinv = row_inv.reshape(-1, 128)
        cinv = col_inv.reshape(-1, 128)
        vmem = pl.BlockSpec(memory_space=pltpu.VMEM)
        hbm = pl.BlockSpec(memory_space=pl.ANY)
        smem = pl.BlockSpec(memory_space=pltpu.SMEM)
        x_part, r_part, s_part = pl.pallas_call(
            functools.partial(_kernel, ring_x, ring_y, rays * ring_y),
            out_shape=(
                jax.ShapeDtypeStruct((GROUPS, ring_y, cy, width), F32),
                jax.ShapeDtypeStruct((GROUPS, ring_x, packed, cols), F32),
                jax.ShapeDtypeStruct((GROUPS, 8, cols), F32),
            ),
            in_specs=[hbm, vmem, hbm, vmem, vmem, smem],
            out_specs=(hbm, hbm, vmem),
            scratch_shapes=[
                pltpu.VMEM((ring_x, 2 * packed, width), BF16),
                pltpu.VMEM((2 * packed, cols), F32),
                pltpu.VMEM((8, (-(-rp // 128) + 1) * 128), F32),
                pltpu.VMEM((packed, cols), F32),
                pltpu.VMEM((cy, width), F32),
                pltpu.VMEM((GROUPS, packed, cols), F32),
                pltpu.VMEM((GROUPS, n_x, packed, cols), F32),
                pltpu.VMEM((GROUPS, n_x, packed, cols), F32),
                pltpu.VMEM((GROUPS, n_x, packed, cols), F32),
                pltpu.VMEM((GROUPS, n_x - 1, packed, cols), F32),
                pltpu.VMEM((GROUPS, ring_x, packed, cols), BF16),
                pltpu.VMEM((GROUPS, ring_x, packed, cols), F32),
                pltpu.VMEM((GROUPS, ring_y, cy, width), F32),
                pltpu.VMEM((GROUPS, ring_y - 1, cy, width), F32),
                pltpu.VMEM((GROUPS, cy, width), F32),
                pltpu.VMEM((GROUPS, ring_y, cy, width), BF16),
                pltpu.VMEM((GROUPS, ring_y, cy, width), F32),
                pltpu.VMEM((GROUPS, 2, width, cols), BF16),
                pltpu.VMEM((GROUPS, 8, cols), F32),
                pltpu.VMEM((ring_x, GROUPS, 8, cols), F32),
                pltpu.VMEM((ring_y, GROUPS, 8, cols), F32),
                pltpu.SemaphoreType.DMA((2, len(CHUNKS), 2)),
                pltpu.SemaphoreType.DMA,
                pltpu.SemaphoreType.DMA,
                pltpu.SemaphoreType.DMA,
                pltpu.SemaphoreType.DMA((192,)),
                pltpu.SemaphoreType.DMA((192,)),
            ],
            compiler_params=pltpu.CompilerParams(
                collective_id=0, has_side_effects=True, vmem_limit_bytes=60 * 1024 * 1024),
        )(a_blk.reshape(ring_x, rp, width), x_loc, sino_loc.reshape(ring_x, rp, cols), rinv, cinv, relaxation.reshape(1))
        step = ring_x // 2
        x_fin, resid, sq = pl.pallas_call(
            _finish,
            grid=(ring_x // step,),
            out_shape=(
                jax.ShapeDtypeStruct((width, cols), F32),
                jax.ShapeDtypeStruct((ring_x, rp, cols), F32),
                jax.ShapeDtypeStruct((SWEEPS, cols), F32),
            ),
            in_specs=[
                pl.BlockSpec((GROUPS, step, packed, cols), lambda i: (0, i, 0, 0)),
                pl.BlockSpec((GROUPS, ring_y, cy, width), lambda i: (0, 0, 0, 0)),
                pl.BlockSpec((GROUPS, 8, cols), lambda i: (0, 0, 0)),
            ],
            out_specs=(
                pl.BlockSpec((width, cols), lambda i: (0, 0)),
                pl.BlockSpec((step, rp, cols), lambda i: (i, 0, 0)),
                pl.BlockSpec((SWEEPS, cols), lambda i: (0, 0)),
            ),
        )(r_part, x_part, s_part)
        return x_fin, resid.reshape(rays, cols), sq

    return jax.shard_map(
        local_sweeps,
        mesh=mesh,
        in_specs=(P("ray", "pix"), P("pix", "part"), P("ray", "part"), P("ray"), P("pix"), P()),
        out_specs=(P("pix", "part"), P("ray", "part"), P(None, "part")),
        check_vma=False,
    )
```
